32 devices in a mesh: wide: 8 (over y, x, core), narrow: 4 (over z).
Axes of the slice: x: 2, y: 2, z: 4, core: 2. Of those that a mesh axis runs over, the one named last changes fastest.
Arguments:
- coefficients: float32 [8, 8192, 8192], P(None, 'wide', 'narrow'), may hold values from -0.07 to 0.07
- tensor_blocks: float32 [8, 32, 8192], P(None, 'wide', 'narrow'), may hold values from -6 to 6
- basis_rows: float32 [32, 8192], P(None, ('wide', 'narrow')), may hold values from -1.1 to 1.1, as said below
Outputs:
- new_basis: float32 [32, 8192], P(None, ('wide', 'narrow'))
- projection: float32 [32, 32], replicated
- factor: float32 [32, 32], replicated
The draws below stay inside these ranges and needn't reach their ends.
Inputs may be any that keep to these rules, and one draw needn't show every extreme that they name: The rows of basis_rows are nearly but not exactly orthonormal: basis_rows basis_rows^T differs from the identity by less than 0.2 in spectral norm.
All inputs are finite; a program needn't handle non-finite values.
Results may differ from the reference program's by a relative error of at most 0.0002.
Values sent between devices are 32-bit elements; how exact they have to be, the bound alone decides.
A program may use at most 128 MiB of HBM per device.

```python
import math
import jax
import jax.numpy as jnp
from jax import lax

N = 8192
K = 8
R = 32
M = 32


def orthonormal_rows(raw):
    hi = lax.Precision.HIGHEST
    for sweep in range(2):
        gram = jnp.dot(raw, raw.T, precision=hi)
        lower = jnp.linalg.cholesky(gram)
        raw = lax.linalg.triangular_solve(lower, raw, left_side=True, lower=True)
    return raw


def coefficient_values(key):
    spread = 0.5 / math.sqrt(K * N)
    inner_key = jax.random.fold_in(key, 11)
    values = jnp.clip(jax.random.normal(inner_key, (K, N, N), jnp.float32), -6.0, 6.0) * spread
    return values


def tensor_values(key):
    inner_key = jax.random.fold_in(key, 12)
    values = jnp.clip(jax.random.normal(inner_key, (K, R, N), jnp.float32), -6.0, 6.0)
    return values


def draw_coefficients(key, part):
    return coefficient_values(key).astype(jnp.float32)


def draw_tensor_blocks(key, part):
    return tensor_values(key).astype(jnp.float32)


def draw_basis_rows(key, part):
    hi = lax.Precision.HIGHEST
    image = jnp.einsum('kic,krc->ir', tensor_values(key), coefficient_values(key), precision=hi)
    noise_key = jax.random.fold_in(key, 13)
    turn_key = jax.random.fold_in(key, 14)
    noise = jax.random.normal(noise_key, (M, N), jnp.float32)
    tilt = 0.06
    frame = orthonormal_rows(image[:M] + 0.1 * noise)
    turn = orthonormal_rows(jax.random.normal(turn_key, (M, M), jnp.float32))
    mixer = jnp.eye(M, dtype=jnp.float32) + tilt * turn
    return jnp.dot(mixer, frame, precision=hi).astype(jnp.float32)


def setup_inputs(seed: int = 0) -> dict:
    seeds = jax.random.split(jax.random.key(seed), 4)
    return {
        "coefficients": draw_coefficients(jax.random.fold_in(seeds[3], 71), 0),
        "tensor_blocks": draw_tensor_blocks(jax.random.fold_in(seeds[3], 71), 0),
        "basis_rows": draw_basis_rows(jax.random.fold_in(seeds[3], 71), 0),
    }


def reference(coefficients, tensor_blocks, basis_rows):
    hi = lax.Precision.HIGHEST
    image = jnp.einsum('kic,krc->ir', tensor_blocks, coefficients, precision=hi)
    first = jnp.dot(basis_rows, image.T, precision=hi)
    once = image - jnp.dot(first.T, basis_rows, precision=hi)
    second = jnp.dot(basis_rows, once.T, precision=hi)
    twice = once - jnp.dot(second.T, basis_rows, precision=hi)
    gram = jnp.dot(twice, twice.T, precision=hi) / N
    factor = jnp.linalg.cholesky(gram)
    new_basis = lax.linalg.triangular_solve(factor, twice, left_side=True, lower=True)
    return (new_basis, first + second, factor)
```

```python
import functools

import jax
import jax.numpy as jnp
from jax import lax
from jax.experimental import pallas as pl
from jax.experimental.pallas import tpu as pltpu
from jax.sharding import PartitionSpec as P

MESH = pl.DeviceIdType.MESH
HI = lax.Precision.HIGHEST
F32 = jnp.float32
DEPTH = 4


def nt(a, b):
    return lax.dot_general(a, b, (((1,), (1,)), ((), ())), precision=HI, preferred_element_type=F32)


def nn(a, b):
    return lax.dot_general(a, b, (((1,), (0,)), ((), ())), precision=HI, preferred_element_type=F32)


def split(x):
    hi = x.astype(jnp.bfloat16)
    return hi, (x - hi.astype(F32)).astype(jnp.bfloat16)


def kernel(wide, narrow, total, coef, tens, basis, out_new, out_proj, out_fac,
           buf, tg, tf, ts, acc, bs, part, img, az1, aw1, az2, aw2,
           csem, lsem, t_send, t_recv, b_send, b_recv, r_send, r_recv,
           z1_send, z1_recv, w1_send, w1_recv, z2_send, z2_recv, w2_send, w2_recv):
    w = lax.axis_index("wide")
    n = lax.axis_index("narrow")
    terms, own, cols = tens.shape
    ranks = own * wide
    rows = basis.shape[1]
    half = wide // 2
    depth = min(DEPTH, terms)
    sib = w + 1 - 2 * lax.rem(w, 2)

    def peer(d):
        return lax.rem(w + 2 * d, wide)

    def sibpeer(d):
        return lax.rem(sib + 2 * d, wide)

    def zpeer(d):
        return lax.rem(n + d, narrow)

    def remote(src, dst, ss, rs, dev):
        return pltpu.make_async_remote_copy(
            src_ref=src, dst_ref=dst, send_sem=ss, recv_sem=rs, device_id=dev, device_id_type=MESH)

    def block(j):
        return lax.rem(n + 1 + j, narrow)

    def load(k, j):
        r0 = pl.multiple_of(block(j) * rows, rows)
        s = lax.rem(k, depth)
        return pltpu.make_async_copy(coef.at[k, pl.ds(r0, rows), :], buf.at[s, j], csem.at[s, j])

    local_t = pltpu.make_async_copy(tens, tg.at[:, w], lsem.at[0])
    local_b = pltpu.make_async_copy(basis, bs.at[n], lsem.at[1])
    local_t.start()
    local_b.start()
    for k in range(depth):
        for j in range(narrow):
            load(k, j).start()

    barrier = pltpu.get_barrier_semaphore()

    @pl.loop(1, wide)
    def _(d):
        pl.semaphore_signal(barrier, inc=1, device_id=(lax.rem(w + d, wide), n), device_id_type=MESH)

    for d in range(1, narrow):
        pl.semaphore_signal(barrier, inc=1, device_id=(w, zpeer(d)), device_id_type=MESH)
    pl.semaphore_wait(barrier, wide - 1 + narrow - 1)

    def t_out(k, d):
        return remote(tg.at[k, w], tg.at[k, w], t_send.at[k, d], t_recv.at[k, w], (peer(d), n))

    def t_sib(k):
        return remote(tg.at[k, w], tg.at[k, w], t_send.at[k, 0], t_recv.at[k, w], (sib, n))

    def t_fwd(k, d):
        p = peer(d)
        return remote(tg.at[k, p], tg.at[k, p], t_send.at[k, half + d], t_recv.at[k, p], (sib, n))

    def t_in(k, p):
        remote(tg.at[k, p], tg.at[k, p], t_send.at[k, 0], t_recv.at[k, p], (sib, n)).wait_recv()

    local_t.wait()

    @pl.loop(0, terms)
    def _(k):
        @pl.loop(1, half)
        def _(d):
            t_out(k, d).start()

        t_sib(k).start()

    local_b.wait()

    def b_out(d):
        return remote(bs.at[n], bs.at[n], b_send.at[d], b_recv.at[n], (w, zpeer(d)))

    for d in range(1, narrow):
        b_out(d).start()

    def forward(k):
        @pl.loop(1, half)
        def _(d):
            t_in(k, peer(d))
            t_fwd(k, d).start()

    def prepare(k):
        @pl.loop(0, half)
        def _(d):
            t_in(k, sibpeer(d))

        for q in range(wide):
            tf[q * own:(q + 1) * own, :] = tg[k, q]
        hi, lo = split(tf[...])
        ts[0:ranks, :] = hi
        ts[ranks:2 * ranks, :] = lo

    def product(s, j):
        hi, lo = split(buf[s, j])
        dims = (((1,), (1,)), ((), ()))
        t = ts[...]
        return (lax.dot_general(hi, t, dims, preferred_element_type=F32)
                + lax.dot_general(lo, t, dims, preferred_element_type=F32))

    acc[...] = jnp.zeros_like(acc)
    forward(0)

    @pl.loop(0, terms - 1)
    def _(k):
        s = lax.rem(k, depth)
        prepare(k)
        group = max(1, narrow // 2)
        for g in range(0, narrow, group):
            for j in range(g, g + group):
                load(k, j).wait()
            for j in range(g, g + group):
                acc[j] += product(s, j)
            for j in range(g, g + group):
                @pl.when(k + depth < terms)
                def _():
                    load(k + depth, j).start()
            if g == 0:
                forward(k + 1)

    last = terms - 1
    prepare(last)
    for d in range(1, narrow):
        q = zpeer(d)
        remote(bs.at[q], bs.at[q], b_send.at[d], b_recv.at[q], (w, q)).wait_recv()
    me = bs[n]
    corr = nt(me, me)

    def r_out(j):
        q = block(j)
        return remote(part.at[j], img.at[n], r_send.at[j], r_recv.at[n], (w, q))

    first_t = jnp.zeros((ranks, bs.shape[1]), F32)
    for j in range(narrow):
        load(last, j).wait()
        v = (acc[j] + product(last % depth, j)).T
        p = v[0:ranks] + v[ranks:2 * ranks]
        if j < narrow - 1:
            part[j] = p
            r_out(j).start()
        else:
            img[n] = p
        first_t = first_t + nt(p, bs[block(j)])

    def all_reduce(value, az, aw, zs, zr, ws, wr):
        az[n] = value

        def z_out(d):
            return remote(az.at[n], az.at[n], zs.at[d], zr.at[n], (w, zpeer(d)))

        for d in range(1, narrow):
            z_out(d).start()
        for d in range(1, narrow):
            q = zpeer(d)
            remote(az.at[q], az.at[q], zs.at[d], zr.at[q], (w, q)).wait_recv()
        t = az[0]
        for q in range(1, narrow):
            t = t + az[q]
        aw[w] = t

        def w_out(d):
            return remote(aw.at[w], aw.at[w], ws.at[d], wr.at[w], (lax.rem(w + d, wide), n))

        for d in range(1, wide):
            w_out(d).start()
        for d in range(1, wide):
            q = lax.rem(w + d, wide)
            remote(aw.at[q], aw.at[q], ws.at[d], wr.at[q], (q, n)).wait_recv()
        t = aw[0]
        for q in range(1, wide):
            t = t + aw[q]

        def finish():
            for d in range(1, narrow):
                z_out(d).wait_send()
            for d in range(1, wide):
                w_out(d).wait_send()

        return t, finish

    m = bs.shape[1]
    both, finish1 = all_reduce(jnp.concatenate([first_t, corr], axis=0), az1, aw1,
                               z1_send, z1_recv, w1_send, w1_recv)
    first_t = both[0:ranks]
    corr = both[ranks:ranks + m]
    proj_t = first_t + (first_t - nn(first_t, corr))
    for d in range(1, narrow):
        q = zpeer(d)
        remote(img.at[q], img.at[q], r_send.at[0], r_recv.at[q], (w, q)).wait_recv()
    image = img[0]
    for q in range(1, narrow):
        image = image + img[q]
    x = image - nn(proj_t, me)
    gram, finish2 = all_reduce(nt(x, x), az2, aw2, z2_send, z2_recv, w2_send, w2_recv)
    a = gram * (1.0 / total)
    sub = lax.broadcasted_iota(jnp.int32, (ranks, 1), 0)
    scale = jnp.ones((ranks, 1), F32)
    for j in range(ranks):
        rs = 1.0 / jnp.sqrt(a[j:j + 1, j:j + 1])
        lcol = jnp.where(sub > j, a[:, j:j + 1] * rs, 0.0)
        arow = a[j:j + 1, :] * rs
        xrow = x[j:j + 1, :] * rs
        scale = jnp.where(sub == j, rs, scale)
        a = a - lcol * arow
        x = x - lcol * xrow
    out_new[...] = x * scale
    upper = a * scale
    r_i = lax.broadcasted_iota(jnp.int32, (ranks, ranks), 0)
    c_i = lax.broadcasted_iota(jnp.int32, (ranks, ranks), 1)
    out_fac[...] = jnp.where(c_i >= r_i, upper, 0.0).T
    out_proj[...] = proj_t.T

    finish1()
    finish2()
    for j in range(narrow - 1):
        r_out(j).wait_send()
    for d in range(1, narrow):
        b_out(d).wait_send()

    @pl.loop(0, terms)
    def _(k):
        t_sib(k).wait_send()

        @pl.loop(1, half)
        def _(d):
            t_out(k, d).wait_send()
            t_fwd(k, d).wait_send()


def body(wide, narrow, total, coefficients, tensor_blocks, basis_rows):
    terms, own, cols = tensor_blocks.shape
    m, rows = basis_rows.shape
    ranks = own * wide
    depth = min(DEPTH, terms)
    dma = lambda *s: pltpu.SemaphoreType.DMA(s)
    vm = lambda s, t=F32: pltpu.VMEM(s, t)
    return pl.pallas_call(
        functools.partial(kernel, wide, narrow, total),
        out_shape=(
            jax.ShapeDtypeStruct((ranks, rows), F32),
            jax.ShapeDtypeStruct((m, ranks), F32),
            jax.ShapeDtypeStruct((ranks, ranks), F32),
        ),
        in_specs=[pl.BlockSpec(memory_space=pl.ANY)] * 3,
        out_specs=[pl.BlockSpec(memory_space=pltpu.VMEM)] * 3,
        scratch_shapes=[
            vm((depth, narrow, rows, cols)),
            vm((terms, wide, own, cols)),
            vm((ranks, cols)),
            vm((2 * ranks, cols), jnp.bfloat16),
            vm((narrow, rows, 2 * ranks)),
            vm((narrow, m, rows)),
            vm((narrow, ranks, rows)),
            vm((narrow, ranks, rows)),
            vm((narrow, ranks + m, m)),
            vm((wide, ranks + m, m)),
            vm((narrow, ranks, ranks)),
            vm((wide, ranks, ranks)),
            dma(depth, narrow), dma(2),
            dma(terms, wide), dma(terms, wide),
            dma(narrow), dma(narrow), dma(narrow), dma(narrow),
            dma(narrow), dma(narrow), dma(wide), dma(wide),
            dma(narrow), dma(narrow), dma(wide), dma(wide),
        ],
        compiler_params=pltpu.CompilerParams(
            collective_id=0, has_side_effects=True, vmem_limit_bytes=60 * 1024 * 1024),
        name="krylov_step",
    )(coefficients, tensor_blocks, basis_rows)


def solution(mesh):
    wide, narrow = mesh.shape["wide"], mesh.shape["narrow"]
    in_specs = (P(None, "wide", "narrow"), P(None, "wide", "narrow"), P(None, ("wide", "narrow")))
    out_specs = (P(None, ("wide", "narrow")), P(), P())

    def whole(coefficients, tensor_blocks, basis_rows):
        total = coefficients.shape[1]
        return jax.shard_map(functools.partial(body, wide, narrow, total), mesh=mesh,
                             in_specs=in_specs, out_specs=out_specs, check_vma=False)(
            coefficients, tensor_blocks, basis_rows)

    return whole
```
